512 devices in a mesh: grp: 2 (over y), ep: 128 (over x, z), tp: 2 (over core).
Axes of the slice: x: 8, y: 2, z: 16, core: 2. Of those that a mesh axis runs over, the one named last changes fastest.
The devices are a block of a 8x8x16 slice.
Arguments:
- queries: bfloat16 [16384, 16, 576], P(('grp', 'ep'), 'tp'), parts along dimension 0, may hold values from -450 to 450
- latent_cache: bfloat16 [768, 512, 576], P(('grp', 'ep'), 'tp'), parts along dimension 0, may hold values from -6 to 6
- residual: bfloat16 [16384, 2048], P(('grp', 'ep')), parts along dimension 0, may hold values from -8 to 8
- token_request: int32 [16384], P(('grp', 'ep')), parts along dimension 0, may hold values from 0 to 2, as said below
- token_visible: int32 [16384], P(('grp', 'ep')), parts along dimension 0, may hold values from 1 to 512, as said below
- value_proj: bfloat16 [16, 512, 128], P('tp', 'ep'), may hold values from -0.25 to 0.25
- out_proj: bfloat16 [2048, 2048], P('tp', 'ep'), may hold values from -0.125 to 0.125
- norm_gain: float32 [2048], replicated, may hold values from 0.1 to 1.9
- router: bfloat16 [2048, 64], replicated, may hold values from -0.0390625 to 0.0390625
- expert_ids: int32 [16384, 6], P(('grp', 'ep')), parts along dimension 0, may hold values from 0 to 63, all different within a row; in each aligned block of 64 rows (0 to 63, 64 to 127, ...) at most 8 rows name the same one
- gate_weight: bfloat16 [128, 2048, 384], P('ep', None, 'tp'), may hold values from -0.125 to 0.125
- up_weight: bfloat16 [128, 2048, 384], P('ep', None, 'tp'), may hold values from -0.125 to 0.125
- down_weight: bfloat16 [128, 384, 2048], P('ep', 'tp'), may hold values from -0.21875 to 0.21875
Outputs:
- hidden: bfloat16 [16384, 2048], P(('grp', 'ep'), 'tp'), parts along dimension 0
- expert_out: bfloat16 [16384, 2048], P(('grp', 'ep'), 'tp'), parts along dimension 0
The draws below stay inside these ranges and needn't reach their ends.
There are 2 independent parts, one for each index of `grp`. The reference program is written for one: setup_inputs(seed, part) draws one part's arguments, and reference() takes and returns one part's arrays. A program takes and returns all parts, laid end to end along the dimension named above; an argument that names none is the same for every part. Nothing has to cross between parts.
Inputs may be any that keep to these rules, and one draw needn't show every extreme that they name: `token_request`: in each ep block, 62 tokens belong to request 0, a prefill span, and each other request has exactly one token; the tokens' order in the block is arbitrary. `token_visible`: the span's tokens read consecutive counts s + 1 to s + 62; 512 is reached in every draw. `expert_ids`: each row names 6 different experts; among the 64 tokens of one ep index no expert is named by more than 8 tokens, and this bound is reached.
All inputs are finite; a program needn't handle non-finite values.
Results may differ from the reference program's by a relative error of at most 0.018.
Values may be sent and summed in bfloat16 or wider, within the bound.
A program may use at most 64 MiB of HBM per device.

```python
import math
import jax
import jax.numpy as jnp
import numpy as np
from jax import lax

D = 2048
HEADS = 16
LATENT = 512
ROPE = 64
VDIM = 128
EXPERTS = 64
TOPK = 6
EXP_HIDDEN = 768
GROUPS = 2
TOK_DEV = 64
REQ_DEV = 3
CACHE_LEN = 512
CAP = 8
PIECES = 128
TOKENS = 8192
REQS = 384
N_EP = 128
N_TP = 2


def request_layout(key):
    blocks = TOKENS // TOK_DEV
    prefill = TOK_DEV - REQ_DEV + 1
    streams = jax.random.split(jax.random.fold_in(key, 101), blocks)

    def one_block(stream, block_index):
        first, second, third = jax.random.split(stream, 3)
        ordering = jax.random.permutation(first, TOK_DEV).astype(jnp.int32)
        span_start = jax.random.randint(second, (), 0, CACHE_LEN - prefill + 1)
        lengths = jax.random.randint(third, (REQ_DEV - 1,), 1, CACHE_LEN + 1)
        lengths = jnp.where((block_index == 0) & (jnp.arange(REQ_DEV - 1) == 0), CACHE_LEN, lengths)
        in_span = ordering < prefill
        request = jnp.where(in_span, 0, ordering - prefill + 1)
        decode_index = jnp.clip(ordering - prefill, 0, REQ_DEV - 2)
        visible = jnp.where(in_span, span_start + ordering + 1, lengths[decode_index])
        return (request.astype(jnp.int32), visible.astype(jnp.int32))
    request, visible = jax.vmap(one_block)(streams, jnp.arange(blocks))
    return (request.reshape(TOKENS), visible.reshape(TOKENS))


def draw_token_request(key, part):
    return request_layout(key)[0]


def draw_token_visible(key, part):
    return request_layout(key)[1]


def cache_rope(key):
    return jnp.clip(jax.random.normal(jax.random.fold_in(key, 202), (REQS, CACHE_LEN, ROPE)), -4.0, 4.0)


def draw_latent_cache(key, part):
    latent = jnp.clip(jax.random.normal(jax.random.fold_in(key, 201), (REQS, CACHE_LEN, LATENT)), -4.0, 4.0)
    return jnp.concatenate([latent, cache_rope(key)], axis=2).astype(jnp.bfloat16)


def draw_queries(key, part):
    shape = (TOKENS, HEADS, LATENT + ROPE)
    values = 0.6 * jnp.clip(jax.random.normal(jax.random.fold_in(key, 301), shape), -4.0, 4.0)
    return values.astype(jnp.bfloat16)


def draw_residual(key, part):
    scales = jnp.exp(jax.random.uniform(jax.random.fold_in(key, 401), (TOKENS, 1), minval=jnp.log(0.2), maxval=jnp.log(2.0)))
    noise = jnp.clip(jax.random.normal(jax.random.fold_in(key, 402), (TOKENS, D)), -4.0, 4.0)
    return (scales * noise).astype(jnp.bfloat16)


def steps_of(own_key, extent, pieces, least, top_value):
    def one(dim, shards_of):
        heights = jax.random.uniform(jax.random.fold_in(jax.random.fold_in(own_key, 6), dim), (shards_of,), jnp.float32, least / len(pieces), top_value / len(pieces))
        return jnp.repeat(jnp.exp(heights), extent[dim] // shards_of).reshape((-1,) + (1,) * (len(extent) - dim - 1))

    level = one(*pieces[0])
    for cut in pieces[1:]:
        level = level * one(*cut)
    return level


def deal_out(stream_key, own, number, rows, count, top, most, skew):
    order = jax.random.permutation(stream_key, count)
    heavy_load, usual = portions_of(count, rows * top, most, skew, True), portions_of(count, rows * top, most, skew, False)
    places = jnp.arange(count)

    def named(tallies, offset_by):
        used = int((tallies > 0).sum())
        fixed = max(1, used // 4)
        moved = fixed + (places - fixed + offset_by * (used - fixed)) % max(1, count - fixed)
        return jnp.zeros((count,), jnp.int32).at[order[jnp.where(places < fixed, places, moved)]].set(jnp.asarray(tallies, jnp.int32))

    tallies = jnp.where(number % 4 == 0, named(heavy_load, number // 4), named(usual, number - number // 4 - 1))
    mixed = jax.random.permutation(jax.random.fold_in(own, 3), count)
    source_of, taker = mixed[0:count // 2 * 2:2], mixed[1:count // 2 * 2:2]
    margin = jnp.minimum(tallies[source_of] - 1, most - tallies[taker]) // 2
    margin = jnp.where((source_of == order[0]) | (taker == order[0]) | (tallies[taker] == 0), 0, jnp.maximum(margin, 0))
    moved = jax.random.randint(jax.random.fold_in(own, 4), (count // 2,), 0, 1 << 20) % (margin + 1)
    tallies = tallies.at[source_of].add(-moved).at[taker].add(moved)
    items = jnp.searchsorted(jnp.cumsum(tallies), jnp.arange(rows * top), side="right").astype(jnp.int32)
    grid = items.reshape(top, rows).T
    grid = grid[jax.random.permutation(jax.random.fold_in(own, 1), rows)]
    offset_by = jax.random.randint(jax.random.fold_in(own, 2), (rows, 1), 0, top)
    return jnp.take_along_axis(grid, (jnp.arange(top)[None, :] + offset_by) % top, axis=1)


def portions_of(amount, total, reach, lean, full):
    loads = [(1 << 20) // math.isqrt(grade ** lean) + 1 for grade in range(1, amount + 1)]
    largest = reach if full else min(reach, max(-(-total // amount), total * loads[0] // sum(loads)))
    least = 1 if total - largest >= amount - 1 else 0
    given, surplus = [largest] + [least] * (amount - 1), total - largest - least * (amount - 1)
    while surplus > 0:
        movable = [i for i in range(1, amount) if given[i] < largest] or [i for i in range(1, amount) if given[i] < reach]
        mass, remaining = sum([loads[i] for i in movable]), surplus
        for i in movable:
            more = min(reach - given[i], max(1, remaining * loads[i] // mass), surplus)
            given[i] = given[i] + more
            surplus = surplus - more
    return np.array(given)


def bell_draw(stream_key, shape, width, most, cuts=(), held_as=jnp.bfloat16):
    gain = steps_of(stream_key, shape, cuts, -0.22, 0.18) if cuts else 1.0
    array = jax.random.normal(stream_key, shape, jnp.float32) * width * gain
    return jnp.minimum(jnp.maximum(array, -most), most).astype(held_as)


def setup_inputs(seed: int = 0, part: int = 0) -> dict:
    key_of = jax.random.split(jax.random.key(seed), 14)
    part_keys = jax.random.split(jax.random.fold_in(key_of[13], part), 14)
    queries = draw_queries(jax.random.fold_in(jax.random.fold_in(key_of[13], part), 71), part)
    latent_cache = draw_latent_cache(jax.random.fold_in(jax.random.fold_in(key_of[13], part), 71), part)
    residual = draw_residual(jax.random.fold_in(jax.random.fold_in(key_of[13], part), 71), part)
    token_request = draw_token_request(jax.random.fold_in(jax.random.fold_in(key_of[13], part), 71), part)
    token_visible = draw_token_visible(jax.random.fold_in(jax.random.fold_in(key_of[13], part), 71), part)
    value_proj = bell_draw(key_of[5], (HEADS, LATENT, VDIM), LATENT ** -0.5, 0.25, ((0, 2), (1, 128)))
    out_proj = bell_draw(key_of[6], (HEADS * VDIM, D), (HEADS * VDIM) ** -0.5, 0.125, ((0, 2), (1, 128)))
    norm_gain = jnp.clip(1.0 + 0.18 * jax.random.normal(key_of[7], (D,), jnp.float32), 0.1, 1.9)
    router = bell_draw(key_of[8], (D, EXPERTS), (12 * D) ** -0.5, 0.0390625)
    expert_ids_keys = jax.random.split(jax.random.fold_in(part_keys[9], 1), TOKENS // TOK_DEV)
    expert_ids_turns = jax.random.permutation(jax.random.fold_in(part_keys[9], 3), TOKENS // TOK_DEV)
    expert_ids = jax.vmap(lambda own, number: deal_out(jax.random.fold_in(part_keys[9], 2), own, number, TOK_DEV, EXPERTS, TOPK, CAP, 2))(expert_ids_keys, expert_ids_turns).reshape((TOKENS, TOPK))
    gate_weight = bell_draw(key_of[10], (PIECES, D, EXP_HIDDEN // GROUPS), D ** -0.5, 0.125, ((0, 128), (2, 2)))
    up_weight = bell_draw(key_of[11], (PIECES, D, EXP_HIDDEN // GROUPS), D ** -0.5, 0.125, ((0, 128), (2, 2)))
    down_weight = bell_draw(key_of[12], (PIECES, EXP_HIDDEN // GROUPS, D), EXP_HIDDEN ** -0.5, 0.21875, ((0, 128), (1, 2)))
    return {"queries": queries, "latent_cache": latent_cache, "residual": residual, "token_request": token_request, "token_visible": token_visible, "value_proj": value_proj, "out_proj": out_proj, "norm_gain": norm_gain, "router": router, "expert_ids": expert_ids, "gate_weight": gate_weight, "up_weight": up_weight, "down_weight": down_weight}


score_scale = 192.0 ** (-0.5)
epsilon = 1e-06

def attend_block(arrays):
    queries, block_rows, token_request, token_visible = arrays
    per_request = block_rows.shape[1]
    flat_rows = block_rows.reshape(-1, block_rows.shape[2]).astype(jnp.float32)
    scores = jnp.einsum('thc,kc->thk', queries.astype(jnp.float32), flat_rows) * score_scale
    column = jnp.arange(flat_rows.shape[0], dtype=jnp.int32)
    owner_id = column // per_request
    position = column % per_request
    allowed = (owner_id[None, :] == token_request[:, None]) & (position[None, :] < token_visible[:, None])
    scores = jnp.where(allowed[:, None, :], scores, -jnp.inf)
    row_peak = lax.optimization_barrier(jnp.max(scores, axis=2, keepdims=True))
    rounded = lax.optimization_barrier(jnp.exp(scores - row_peak).astype(jnp.bfloat16))
    weights = rounded.astype(jnp.float32)
    totals = lax.optimization_barrier(jnp.sum(weights, axis=2, keepdims=True))
    summed = jnp.einsum('thk,kc->thc', weights, flat_rows[:, :LATENT])
    return (summed / totals).astype(jnp.bfloat16)

def reference(queries, latent_cache, residual, token_request, token_visible, value_proj, out_proj, norm_gain, router, expert_ids, gate_weight, up_weight, down_weight):
    blocks = TOKENS // TOK_DEV
    context = lax.map(attend_block, (queries.reshape(blocks, TOK_DEV, HEADS, LATENT + ROPE), latent_cache.reshape(blocks, REQ_DEV, CACHE_LEN, LATENT + ROPE), token_request.reshape(blocks, TOK_DEV), token_visible.reshape(blocks, TOK_DEV)))
    context = context.reshape(TOKENS, HEADS, LATENT)
    heads_out = jnp.einsum('thl,hlv->thv', context.astype(jnp.float32), value_proj.astype(jnp.float32)).astype(jnp.bfloat16)
    heads_out = heads_out.reshape(TOKENS, HEADS * VDIM)
    attention = jnp.dot(heads_out, out_proj, preferred_element_type=jnp.float32)
    hidden = (residual.astype(jnp.float32) + attention).astype(jnp.bfloat16)
    hidden_wide = hidden.astype(jnp.float32)
    normed = (hidden_wide * lax.rsqrt(lax.optimization_barrier(jnp.mean(hidden_wide * hidden_wide, axis=1, keepdims=True)) + epsilon) * norm_gain).astype(jnp.bfloat16)
    logits = jnp.dot(normed, router, preferred_element_type=jnp.float32)
    gate_share = jax.nn.softmax(jnp.take_along_axis(logits, expert_ids, axis=1), axis=1).astype(jnp.bfloat16)
    flat_ids = expert_ids.reshape(-1)
    flat_share = gate_share.reshape(-1).astype(jnp.float32)
    bound = N_EP * CAP
    part_width = EXP_HIDDEN // (GROUPS * N_TP)

    def piece_step(running, piece_index):
        expert = piece_index // GROUPS
        hit_mask = flat_ids == expert
        hits = jnp.nonzero(hit_mask, size=bound, fill_value=0)[0].astype(jnp.int32)
        live = jnp.arange(bound, dtype=jnp.int32) < jnp.sum(hit_mask.astype(jnp.int32))
        token_rows = hits // TOPK
        picked = normed[token_rows]
        gate_vals = jnp.dot(picked, gate_weight[piece_index], preferred_element_type=jnp.float32)
        up_vals = jnp.dot(picked, up_weight[piece_index], preferred_element_type=jnp.float32)
        activated = (jax.nn.silu(gate_vals) * up_vals).astype(jnp.bfloat16)
        combined = jnp.zeros((bound, D), jnp.float32)
        for half_index in range(N_TP):
            lower = half_index * part_width
            piece_out = jnp.dot(activated[:, lower:lower + part_width], down_weight[piece_index, lower:lower + part_width], preferred_element_type=jnp.float32).astype(jnp.bfloat16)
            combined = combined + piece_out.astype(jnp.float32)
        scaled = combined * jnp.where(live, flat_share[hits], 0.0)[:, None]
        return (running.at[token_rows].add(scaled), None)
    routed, _ = lax.scan(piece_step, jnp.zeros((TOKENS, D), jnp.float32), jnp.arange(PIECES, dtype=jnp.int32))
    return (hidden, routed.astype(jnp.bfloat16))
```

```python
import jax
import jax.numpy as jnp
from jax import lax
from jax.experimental import pallas as pl
from jax.experimental.pallas import tpu as pltpu
from jax.sharding import Mesh
from jax.sharding import PartitionSpec as P

LATENT = 512
VDIM = 128
EXPERTS = 64
TOPK = 6
GROUPS = 2
CAP = 8
PIECES = 128
MESH = pl.DeviceIdType.MESH
EP = ("ep_0", "ep_1")
GRP_EP = ("grp", "ep_0", "ep_1")


score_scale = 192.0 ** (-0.5)
epsilon = 1e-06


def from_everyone(value, axis):
    peers = lax.axis_size(axis)
    return lax.all_to_all(
        jnp.broadcast_to(value[None], (peers, *value.shape)), axis, 0, 0, tiled=True
    )


def laid_out(pieces, dim):
    lengths = list(pieces.shape[1:])
    lengths[dim] *= pieces.shape[0]
    return jnp.moveaxis(pieces, 0, dim).reshape(lengths)


def collect(value, axis, dim):
    pieces = from_everyone(value, axis)
    return laid_out(pieces, dim)


def of_everyone(value, axis):
    return from_everyone(value, axis).max(axis=0)


def split_up(value, dim, peers):
    before, after = (value.shape[:dim], value.shape[dim + 1 :])
    return jnp.moveaxis(value.reshape(*before, peers, -1, *after), dim, 0)


def sent_and_summed(value, axis, dim):
    peers = lax.axis_size(axis)
    pieces = lax.all_to_all(split_up(value, dim, peers), axis, 0, 0, tiled=True)
    return jnp.sum(pieces, axis=0)


def sent_together(arrays, axis, dim, along):
    columns = [a.reshape(*a.shape[:along], -1) for a in arrays]
    both = jnp.concatenate(columns, axis=along)
    result, at, outs = (sent_and_summed(both, axis, dim), 0, [])
    for a, column in zip(arrays, columns):
        piece = result[..., at : at + column.shape[along]]
        outs.append(piece.reshape(*piece.shape[:along], *a.shape[along:]))
        at += column.shape[along]
    return tuple(outs)


def stacked_from(value, axes, order):
    pieces = value[None]
    for k in order:
        pieces = lax.all_gather(pieces, axes[k], axis=0, tiled=True)
    carried = [lax.axis_size(axes[k]) for k in reversed(order)]
    pieces = pieces.reshape(*carried, *value.shape)
    turned = sorted(range(len(order)), key=lambda place: order[len(order) - 1 - place])
    return pieces.transpose(*turned, *range(len(order), pieces.ndim)).reshape(-1, *value.shape)


def whole_of(value, axes, order, dim):
    return laid_out(stacked_from(value, axes, order), dim)


def over_copies(value, axis):
    everything = from_everyone(value, axis)
    return jnp.sum(everything, axis=0)


def masked_scores(queries, block_rows, token_request, token_visible, offset):
    per_request = block_rows.shape[1]
    flat_rows = block_rows.reshape(-1, block_rows.shape[2])
    scores = (
        jnp.einsum("thc,kc->thk", queries, flat_rows, preferred_element_type=jnp.float32)
        * score_scale
    )
    column = jnp.arange(flat_rows.shape[0], dtype=jnp.int32)
    owner_id = column // per_request
    position = column % per_request + offset
    allowed = (owner_id[None, :] == token_request[:, None]) & (
        position[None, :] < token_visible[:, None]
    )
    return (jnp.where(allowed[:, None, :], scores, -jnp.inf), flat_rows)


def weighted_rows(scores, row_peak, flat_rows):
    weights = jnp.exp(scores - row_peak[:, :, None]).astype(jnp.bfloat16)
    totals = jnp.sum(weights.astype(jnp.float32), axis=2)
    summed = jnp.einsum(
        "thk,kc->thc", weights, flat_rows[:, :LATENT], preferred_element_type=jnp.float32
    )
    return (summed, totals)


def ring_ids(axis):
    size = lax.axis_size(axis)
    me = lax.axis_index(axis)
    return me, lax.rem(me + 1, size), lax.rem(me + size - 1, size), size


def wait_bytes(view, sem):
    pltpu.make_async_copy(view, view, sem).wait()


def moe_kernel(
    meta_ref, tok_ref, gate_ref, up_ref, down_ref, out_ref,
    blk, met, mix, picked, rows, rowsx, act, actx, downx, outs, ret, rss, rsl, rsr,
    ag_s, ag_r, am_s, am_r, x_s, x_r, d_s, d_r, a_s, a_r, w_s, w_r, t_s, t_r, rs_s, rs_r,
):
    x, _, _, nx = ring_ids("ep_0")
    z, right, left, nz = ring_ids("ep_1")
    core = lax.axis_index("tp")
    other = 1 - core
    steps = nz // 2
    toks, half = tok_ref.shape
    rows_n = nx * 2 * CAP

    barrier = pltpu.get_barrier_semaphore()
    for name, peer in (("ep_1", left), ("ep_1", right), ("tp", other)):
        pl.semaphore_signal(barrier, inc=1, device_id={name: peer}, device_id_type=MESH)
    for j in range(1, nx):
        pl.semaphore_signal(
            barrier, inc=1, device_id={"ep_0": lax.rem(x + j, nx)}, device_id_type=MESH
        )
    pl.semaphore_wait(barrier, 3 + nx - 1)

    def remote(src, dst, ssem, rsem, axis, peer):
        return pltpu.make_async_remote_copy(
            src_ref=src, dst_ref=dst, send_sem=ssem, recv_sem=rsem,
            device_id={axis: peer}, device_id_type=MESH,
        )

    def gather_copy(src, slot, side, what):
        ssem, rsem = (ag_s, ag_r) if what is blk else (am_s, am_r)
        peer = right if side == 0 else left
        return remote(
            src, what.at[slot, side], ssem.at[slot, side], rsem.at[slot, side], "ep_1", peer
        )

    for side, slot in ((0, 0), (1, 1)):
        gather_copy(meta_ref, slot, side, met).start()
        gather_copy(tok_ref, slot, side, blk).start()
    mine = pl.ds(pl.multiple_of(core * half, half), half)
    theirs = pl.ds(pl.multiple_of(other * half, half), half)
    swap = remote(down_ref.at[:, theirs], downx, w_s, w_r, "tp", other)
    swap.start()
    blk[0, 1] = tok_ref[...]
    met[0, 1] = meta_ref[...]

    row = lax.broadcasted_iota(jnp.int32, (rows_n, 2 * toks), 0)
    lane = lax.broadcasted_iota(jnp.int32, (rows_n, 2 * toks), 1)
    side_of_row = (row // CAP) % 2
    expert = (row // (2 * CAP)) * (nz // 2) + z // 2
    want = jnp.where(side_of_row == lane // toks, expert * CAP + row % CAP, -1).astype(jnp.float32)
    first_half = lax.broadcasted_iota(jnp.int32, (16, 2 * toks), 1) < toks

    def pick(g):
        both = jnp.where(first_half, met[g, 0], met[g, 1])
        share = jnp.zeros((rows_n, 2 * toks), jnp.float32)
        chosen = jnp.zeros((rows_n, 2 * toks), jnp.float32)
        for k in range(TOPK):
            same = want == both[k : k + 1, :]
            share = share + jnp.where(same, both[8 + k : 9 + k, :], 0.0)
            chosen = chosen + jnp.where(same, 1.0, 0.0)
        mix[g] = share.T.astype(jnp.bfloat16)
        tokens = blk[g].reshape(2 * toks, half)
        got = jnp.dot(chosen.astype(jnp.bfloat16), tokens, preferred_element_type=jnp.float32)
        picked[g] = got.astype(jnp.bfloat16).reshape(nx, 2 * CAP, half)
        rows[g, x] = picked[g, x]
        for j in range(1, nx):
            peer = lax.rem(x + j, nx)
            remote(picked.at[g, peer], rows.at[g, x], x_s.at[g], x_r.at[g], "ep_0", peer).start()

    def stage_gather(g):
        gather_copy(met.at[0, 0], g, 0, met).wait_recv()
        gather_copy(blk.at[0, 0], g, 0, blk).wait_recv()

        @pl.when(g > 0)
        def _():
            gather_copy(met.at[0, 0], g, 1, met).wait_recv()
            gather_copy(blk.at[0, 0], g, 1, blk).wait_recv()

        @pl.when(g < steps - 1)
        def _():
            gather_copy(met.at[g, 0], g + 1, 0, met).start()
            gather_copy(blk.at[g, 0], g + 1, 0, blk).start()

        @pl.when((g > 0) & (g < steps - 1))
        def _():
            gather_copy(met.at[g, 1], g + 1, 1, met).start()
            gather_copy(blk.at[g, 1], g + 1, 1, blk).start()

        pick(g)

    def rows_swap(g):
        return remote(rows.at[g], rowsx.at[g], d_s.at[g], d_r.at[g], "tp", other)

    def act_swap(g):
        return remote(act.at[g], actx.at[g], a_s.at[g], a_r.at[g], "tp", other)

    def stage_arrive(g):
        wait_bytes(rows.at[g, pl.ds(0, nx - 1)], x_r.at[g])
        rows_swap(g).start()

    def stage_up(g):
        rows_swap(g).wait_recv()
        here = rows[g].reshape(rows_n, half)
        there = rowsx[g].reshape(rows_n, half)

        def into(weight):
            return jnp.dot(here, weight[mine, :], preferred_element_type=jnp.float32) + jnp.dot(
                there, weight[theirs, :], preferred_element_type=jnp.float32
            )

        gate_vals = into(gate_ref)
        up_vals = into(up_ref)
        act[g] = (gate_vals / (1.0 + jnp.exp(-gate_vals)) * up_vals).astype(jnp.bfloat16)
        act_swap(g).start()

    def stage_down(g):
        act_swap(g).wait_recv()
        total = jnp.dot(act[g], down_ref[:, mine], preferred_element_type=jnp.float32)
        total = total + jnp.dot(actx[g], downx[...], preferred_element_type=jnp.float32)
        outs[g] = total.astype(jnp.bfloat16).reshape(nx, 2 * CAP, half)

    def tick(t, carry):
        @pl.when(t < steps)
        def _():
            stage_gather(t)

        @pl.when((t >= 1) & (t < steps + 1))
        def _():
            stage_arrive(t - 1)

        @pl.when((t >= 2) & (t < steps + 2))
        def _():
            stage_up(t - 2)

        @pl.when(t >= 3)
        def _():
            stage_down(t - 3)

        return carry

    swap.wait_recv()
    lax.fori_loop(0, steps + 3, tick, 0)

    def send_back(i, carry):
        g = steps - 1 - i
        ret[g, x] = outs[g, x]
        for j in range(1, nx):
            peer = lax.rem(x + j, nx)
            remote(outs.at[g, peer], ret.at[g, x], t_s.at[g], t_r.at[g], "ep_0", peer).start()
        return carry

    lax.fori_loop(0, steps, send_back, 0)

    def left_copy(g):
        return remote(rss.at[g, 0], rsl.at[g], rs_s.at[g, 0], rs_r.at[g, 0], "ep_1", left)

    def right_copy(g):
        return remote(rss.at[g, 1], rsr.at[g], rs_s.at[g, 1], rs_r.at[g, 1], "ep_1", right)

    def mixed(g):
        wait_bytes(ret.at[g, pl.ds(0, nx - 1)], t_r.at[g])
        return jnp.dot(
            mix[g], ret[g].reshape(rows_n, half), preferred_element_type=jnp.float32
        )

    def combine(i, carry):
        g = steps - 1 - i
        part = mixed(g)

        @pl.when(i == 0)
        def _():
            rss[g, 0] = part[:toks].astype(jnp.bfloat16)
            rss[g, 1] = part[toks:].astype(jnp.bfloat16)

        @pl.when(i > 0)
        def _():
            left_copy(g + 1).wait_recv()
            right_copy(g + 1).wait_recv()
            rss[g, 0] = (part[:toks] + rsl[g + 1].astype(jnp.float32)).astype(jnp.bfloat16)
            rss[g, 1] = (part[toks:] + rsr[g + 1].astype(jnp.float32)).astype(jnp.bfloat16)

        left_copy(g).start()
        right_copy(g).start()
        return carry

    lax.fori_loop(0, steps - 1, combine, 0)
    part = mixed(0)
    left_copy(1).wait_recv()
    right_copy(1).wait_recv()
    rss[0, 0] = (part[:toks] + rsl[1].astype(jnp.float32)).astype(jnp.bfloat16)
    left_copy(0).start()
    total = part[toks:] + rsr[1].astype(jnp.float32)
    left_copy(0).wait_recv()
    out_ref[...] = (total + rsl[0].astype(jnp.float32)).astype(jnp.bfloat16)

    swap.wait_send()

    def drain(g, carry):
        wait_bytes(picked.at[g, pl.ds(0, nx - 1)], x_s.at[g])
        wait_bytes(outs.at[g, pl.ds(0, nx - 1)], t_s.at[g])
        rows_swap(g).wait_send()
        act_swap(g).wait_send()
        gather_copy(met.at[0, 0], g, 0, met).wait_send()
        gather_copy(blk.at[0, 0], g, 0, blk).wait_send()
        left_copy(g).wait_send()

        @pl.when(g > 0)
        def _():
            gather_copy(met.at[0, 0], g, 1, met).wait_send()
            gather_copy(blk.at[0, 0], g, 1, blk).wait_send()
            right_copy(g).wait_send()

        return carry

    lax.fori_loop(0, steps, drain, 0)


def routed_experts(meta, tokens, gate_weight, up_weight, down_weight):
    toks, half = tokens.shape
    nx, nz = lax.axis_size("ep_0"), lax.axis_size("ep_1")
    steps, hidden = nz // 2, gate_weight.shape[1]
    rows_n = nx * 2 * CAP
    bf = jnp.bfloat16
    group = (steps, nx, 2 * CAP, half)
    dma = pltpu.SemaphoreType.DMA
    return pl.pallas_call(
        moe_kernel,
        out_shape=jax.ShapeDtypeStruct((toks, half), bf),
        in_specs=[pl.BlockSpec(memory_space=pltpu.VMEM)] * 5,
        out_specs=pl.BlockSpec(memory_space=pltpu.VMEM),
        scratch_shapes=[
            pltpu.VMEM((steps, 2, toks, half), bf),
            pltpu.VMEM((steps, 2, 16, 2 * toks), jnp.float32),
            pltpu.VMEM((steps, 2 * toks, rows_n), bf),
            pltpu.VMEM(group, bf),
            pltpu.VMEM(group, bf),
            pltpu.VMEM(group, bf),
            pltpu.VMEM((steps, rows_n, hidden), bf),
            pltpu.VMEM((steps, rows_n, hidden), bf),
            pltpu.VMEM((hidden, half), bf),
            pltpu.VMEM(group, bf),
            pltpu.VMEM(group, bf),
            pltpu.VMEM((steps, 2, toks, half), bf),
            pltpu.VMEM((steps, toks, half), bf),
            pltpu.VMEM((steps, toks, half), bf),
            dma((steps, 2)), dma((steps, 2)), dma((steps, 2)), dma((steps, 2)),
            dma((steps,)), dma((steps,)), dma((steps,)), dma((steps,)),
            dma((steps,)), dma((steps,)), dma, dma,
            dma((steps,)), dma((steps,)), dma((steps, 2)), dma((steps, 2)),
        ],
        compiler_params=pltpu.CompilerParams(
            collective_id=1, has_side_effects=True, vmem_limit_bytes=60 * 2**20
        ),
        name="routed_experts",
    )(meta, tokens, gate_weight, up_weight, down_weight)


def routing_table(logits, expert_ids):
    tokens, top = expert_ids.shape
    experts = jnp.arange(logits.shape[1], dtype=jnp.int32)
    named = expert_ids[:, :, None] == experts[None, None, :]
    chosen = jnp.sum(jnp.where(named, logits[:, None, :], 0.0), axis=2)
    gate_share = jax.nn.softmax(chosen, axis=1).astype(jnp.bfloat16).astype(jnp.float32)
    counts = jnp.sum(named.astype(jnp.float32), axis=1)
    token = jnp.arange(tokens, dtype=jnp.int32)
    before = (token[None, :] < token[:, None]).astype(jnp.float32)
    earlier = jnp.dot(before, counts, preferred_element_type=jnp.float32)
    place = jnp.sum(jnp.where(named, earlier[:, None, :], 0.0), axis=2)
    slot = expert_ids.astype(jnp.float32) * CAP + place
    fill = jnp.zeros((tokens, 8 - top), jnp.float32)
    table = jnp.concatenate([slot, fill - 2.0, gate_share, fill], axis=1).T
    return jnp.concatenate([table, table], axis=1)


def body(
    queries,
    latent_cache,
    residual,
    token_request,
    token_visible,
    value_proj,
    out_proj,
    norm_gain,
    router,
    expert_ids,
    gate_weight,
    up_weight,
    down_weight,
):
    all_heads = collect(queries, "tp", 1)
    offset = lax.axis_index("tp") * latent_cache.shape[1]
    scores, flat_rows = masked_scores(all_heads, latent_cache, token_request, token_visible, offset)
    row_peak = of_everyone(jnp.max(scores, axis=2), "tp")
    part_sum, part_total = weighted_rows(scores, row_peak, flat_rows)
    summed, totals = sent_together((part_sum, part_total), "tp", 1, 2)
    context = (summed / totals[:, :, None]).astype(jnp.bfloat16)
    tokens_here = context.shape[0]
    heads_here = context.shape[1]
    head_values = jnp.einsum(
        "thl,hlv->thv",
        context,
        whole_of(value_proj, EP, (0, 1), 1),
        preferred_element_type=jnp.float32,
    )
    heads_out = head_values.astype(jnp.bfloat16).reshape(tokens_here, heads_here * VDIM)
    attention_part = jnp.dot(
        heads_out, whole_of(out_proj, EP, (0, 1), 1), preferred_element_type=jnp.float32
    )
    attention = over_copies(attention_part, "tp")
    hidden = (residual.astype(jnp.float32) + attention).astype(jnp.bfloat16)
    hidden_wide = hidden.astype(jnp.float32)
    normed = (
        hidden_wide
        * lax.rsqrt(jnp.mean(hidden_wide * hidden_wide, axis=1, keepdims=True) + epsilon)
        * norm_gain
    ).astype(jnp.bfloat16)
    logits = jnp.dot(normed, router, preferred_element_type=jnp.float32)
    meta = routing_table(logits, expert_ids)
    half_width = normed.shape[1] // lax.axis_size("tp")
    core_start = lax.axis_index("tp") * half_width
    normed_share = lax.dynamic_slice_in_dim(normed, core_start, half_width, 1)
    expert_out = routed_experts(
        meta, normed_share, gate_weight[0], up_weight[0], down_weight[0]
    )
    hidden_part = lax.dynamic_slice_in_dim(hidden, core_start, half_width, 1)
    return (hidden_part, expert_out)


def solution(mesh):
    finer = Mesh(
        mesh.devices.reshape(mesh.shape["grp"], 8, 16, mesh.shape["tp"]),
        ("grp", "ep_0", "ep_1", "tp"),
    )
    in_specs = (
        P(GRP_EP, "tp", None),
        P(GRP_EP, "tp", None),
        P(GRP_EP, None),
        P(GRP_EP),
        P(GRP_EP),
        P("tp", EP, None),
        P("tp", EP),
        P(),
        P(),
        P(GRP_EP, None),
        P(EP, None, "tp"),
        P(EP, None, "tp"),
        P(EP, "tp", None),
    )
    out_specs = (P(GRP_EP, "tp"), P(GRP_EP, "tp"))
    return jax.shard_map(body, mesh=finer, in_specs=in_specs, out_specs=out_specs, check_vma=False)
```

```python
import functools

import jax
import jax.numpy as jnp
from jax import lax
from jax.experimental import pallas as pl
from jax.experimental.pallas import tpu as pltpu
from jax.sharding import Mesh
from jax.sharding import PartitionSpec as P


MESH = pl.DeviceIdType.MESH
VDIM = 128
TOPK = 6
CAP = 8
EP = ("ep_0", "ep_1")
GRP_EP = ("grp", "ep_0", "ep_1")


score_scale = 192.0 ** (-0.5)
epsilon = 1e-06


def ring_ids(axis):
    size = lax.axis_size(axis)
    me = lax.axis_index(axis)
    return me, lax.rem(me + 1, size), lax.rem(me + size - 1, size), size


def wait_bytes(view, sem):
    pltpu.make_async_copy(view, view, sem).wait()


def moe_kernel(
    meta_ref, tok_ref, gate_ref, up_ref, down_ref, out_ref,
    blk, met, mix, picked, rows, rowsx, act, actx, downx, outs, ret, rss, rsl, rsr,
    ag_s, ag_r, am_s, am_r, x_s, x_r, d_s, d_r, a_s, a_r, w_s, w_r, t_s, t_r, rs_s, rs_r,
):
    x, _, _, nx = ring_ids("ep_0")
    z, right, left, nz = ring_ids("ep_1")
    core = lax.axis_index("tp")
    other = 1 - core
    steps = nz // 2
    toks, half = tok_ref.shape
    rows_n = nx * 2 * CAP

    barrier = pltpu.get_barrier_semaphore()
    for name, peer in (("ep_1", left), ("ep_1", right), ("tp", other)):
        pl.semaphore_signal(barrier, inc=1, device_id={name: peer}, device_id_type=MESH)
    for j in range(1, nx):
        pl.semaphore_signal(
            barrier, inc=1, device_id={"ep_0": lax.rem(x + j, nx)}, device_id_type=MESH
        )
    pl.semaphore_wait(barrier, 3 + nx - 1)

    def remote(src, dst, ssem, rsem, axis, peer):
        return pltpu.make_async_remote_copy(
            src_ref=src, dst_ref=dst, send_sem=ssem, recv_sem=rsem,
            device_id={axis: peer}, device_id_type=MESH,
        )

    def gather_copy(src, slot, side, what):
        ssem, rsem = (ag_s, ag_r) if what is blk else (am_s, am_r)
        peer = right if side == 0 else left
        return remote(
            src, what.at[slot, side], ssem.at[slot, side], rsem.at[slot, side], "ep_1", peer
        )

    for side, slot in ((0, 0), (1, 1)):
        gather_copy(meta_ref, slot, side, met).start()
        gather_copy(tok_ref, slot, side, blk).start()
    mine = pl.ds(pl.multiple_of(core * half, half), half)
    theirs = pl.ds(pl.multiple_of(other * half, half), half)
    swap = remote(down_ref.at[:, theirs], downx, w_s, w_r, "tp", other)
    swap.start()
    blk[0, 1] = tok_ref[...]
    met[0, 1] = meta_ref[...]

    row = lax.broadcasted_iota(jnp.int32, (rows_n, 2 * toks), 0)
    lane = lax.broadcasted_iota(jnp.int32, (rows_n, 2 * toks), 1)
    side_of_row = (row // CAP) % 2
    expert = (row // (2 * CAP)) * (nz // 2) + z // 2
    want = jnp.where(side_of_row == lane // toks, expert * CAP + row % CAP, -1).astype(jnp.float32)
    first_half = lax.broadcasted_iota(jnp.int32, (16, 2 * toks), 1) < toks

    def pick(g):
        both = jnp.where(first_half, met[g, 0], met[g, 1])
        share = jnp.zeros((rows_n, 2 * toks), jnp.float32)
        chosen = jnp.zeros((rows_n, 2 * toks), jnp.float32)
        for k in range(TOPK):
            same = want == both[k : k + 1, :]
            share = share + jnp.where(same, both[8 + k : 9 + k, :], 0.0)
            chosen = chosen + jnp.where(same, 1.0, 0.0)
        mix[g] = share.T.astype(jnp.bfloat16)
        tokens = blk[g].reshape(2 * toks, half)
        got = jnp.dot(chosen.astype(jnp.bfloat16), tokens, preferred_element_type=jnp.float32)
        picked[g] = got.astype(jnp.bfloat16).reshape(nx, 2 * CAP, half)
        rows[g, x] = picked[g, x]
        for j in range(1, nx):
            peer = lax.rem(x + j, nx)
            remote(picked.at[g, peer], rows.at[g, x], x_s.at[g], x_r.at[g], "ep_0", peer).start()

    def stage_gather(g):
        gather_copy(met.at[0, 0], g, 0, met).wait_recv()
        gather_copy(blk.at[0, 0], g, 0, blk).wait_recv()

        @pl.when(g > 0)
        def _():
            gather_copy(met.at[0, 0], g, 1, met).wait_recv()
            gather_copy(blk.at[0, 0], g, 1, blk).wait_recv()

        @pl.when(g < steps - 1)
        def _():
            gather_copy(met.at[g, 0], g + 1, 0, met).start()
            gather_copy(blk.at[g, 0], g + 1, 0, blk).start()

        @pl.when((g > 0) & (g < steps - 1))
        def _():
            gather_copy(met.at[g, 1], g + 1, 1, met).start()
            gather_copy(blk.at[g, 1], g + 1, 1, blk).start()

        pick(g)

    def rows_swap(g):
        return remote(rows.at[g], rowsx.at[g], d_s.at[g], d_r.at[g], "tp", other)

    def act_swap(g):
        return remote(act.at[g], actx.at[g], a_s.at[g], a_r.at[g], "tp", other)

    def stage_arrive(g):
        wait_bytes(rows.at[g, pl.ds(0, nx - 1)], x_r.at[g])
        rows_swap(g).start()

    def stage_up(g):
        rows_swap(g).wait_recv()
        here = rows[g].reshape(rows_n, half)
        there = rowsx[g].reshape(rows_n, half)

        def into(weight):
            return jnp.dot(here, weight[mine, :], preferred_element_type=jnp.float32) + jnp.dot(
                there, weight[theirs, :], preferred_element_type=jnp.float32
            )

        gate_vals = into(gate_ref)
        up_vals = into(up_ref)
        act[g] = (gate_vals / (1.0 + jnp.exp(-gate_vals)) * up_vals).astype(jnp.bfloat16)
        act_swap(g).start()

    def stage_down(g):
        act_swap(g).wait_recv()
        total = jnp.dot(act[g], down_ref[:, mine], preferred_element_type=jnp.float32)
        total = total + jnp.dot(actx[g], downx[...], preferred_element_type=jnp.float32)
        outs[g] = total.astype(jnp.bfloat16).reshape(nx, 2 * CAP, half)

    def tick(t, carry):
        @pl.when(t < steps)
        def _():
            stage_gather(t)

        @pl.when((t >= 1) & (t < steps + 1))
        def _():
            stage_arrive(t - 1)

        @pl.when((t >= 2) & (t < steps + 2))
        def _():
            stage_up(t - 2)

        @pl.when(t >= 3)
        def _():
            stage_down(t - 3)

        return carry

    swap.wait_recv()
    lax.fori_loop(0, steps + 3, tick, 0)

    def send_back(i, carry):
        g = steps - 1 - i
        ret[g, x] = outs[g, x]
        for j in range(1, nx):
            peer = lax.rem(x + j, nx)
            remote(outs.at[g, peer], ret.at[g, x], t_s.at[g], t_r.at[g], "ep_0", peer).start()
        return carry

    lax.fori_loop(0, steps, send_back, 0)

    def left_copy(g):
        return remote(rss.at[g, 0], rsl.at[g], rs_s.at[g, 0], rs_r.at[g, 0], "ep_1", left)

    def right_copy(g):
        return remote(rss.at[g, 1], rsr.at[g], rs_s.at[g, 1], rs_r.at[g, 1], "ep_1", right)

    def mixed(g):
        wait_bytes(ret.at[g, pl.ds(0, nx - 1)], t_r.at[g])
        return jnp.dot(
            mix[g], ret[g].reshape(rows_n, half), preferred_element_type=jnp.float32
        )

    def combine(i, carry):
        g = steps - 1 - i
        part = mixed(g)

        @pl.when(i == 0)
        def _():
            rss[g, 0] = part[:toks].astype(jnp.bfloat16)
            rss[g, 1] = part[toks:].astype(jnp.bfloat16)

        @pl.when(i > 0)
        def _():
            left_copy(g + 1).wait_recv()
            right_copy(g + 1).wait_recv()
            rss[g, 0] = (part[:toks] + rsl[g + 1].astype(jnp.float32)).astype(jnp.bfloat16)
            rss[g, 1] = (part[toks:] + rsr[g + 1].astype(jnp.float32)).astype(jnp.bfloat16)

        left_copy(g).start()
        right_copy(g).start()
        return carry

    lax.fori_loop(0, steps - 1, combine, 0)
    part = mixed(0)
    left_copy(1).wait_recv()
    right_copy(1).wait_recv()
    rss[0, 0] = (part[:toks] + rsl[1].astype(jnp.float32)).astype(jnp.bfloat16)
    left_copy(0).start()
    total = part[toks:] + rsr[1].astype(jnp.float32)
    left_copy(0).wait_recv()
    out_ref[...] = (total + rsl[0].astype(jnp.float32)).astype(jnp.bfloat16)

    swap.wait_send()

    def drain(g, carry):
        wait_bytes(picked.at[g, pl.ds(0, nx - 1)], x_s.at[g])
        wait_bytes(outs.at[g, pl.ds(0, nx - 1)], t_s.at[g])
        rows_swap(g).wait_send()
        act_swap(g).wait_send()
        gather_copy(met.at[0, 0], g, 0, met).wait_send()
        gather_copy(blk.at[0, 0], g, 0, blk).wait_send()
        left_copy(g).wait_send()

        @pl.when(g > 0)
        def _():
            gather_copy(met.at[0, 0], g, 1, met).wait_send()
            gather_copy(blk.at[0, 0], g, 1, blk).wait_send()
            right_copy(g).wait_send()

        return carry

    lax.fori_loop(0, steps, drain, 0)


def routed_experts(meta, tokens, gate_weight, up_weight, down_weight):
    toks, half = tokens.shape
    nx, nz = lax.axis_size("ep_0"), lax.axis_size("ep_1")
    steps, hidden = nz // 2, gate_weight.shape[1]
    rows_n = nx * 2 * CAP
    bf = jnp.bfloat16
    group = (steps, nx, 2 * CAP, half)
    dma = pltpu.SemaphoreType.DMA
    return pl.pallas_call(
        moe_kernel,
        out_shape=jax.ShapeDtypeStruct((toks, half), bf),
        in_specs=[pl.BlockSpec(memory_space=pltpu.VMEM)] * 5,
        out_specs=pl.BlockSpec(memory_space=pltpu.VMEM),
        scratch_shapes=[
            pltpu.VMEM((steps, 2, toks, half), bf),
            pltpu.VMEM((steps, 2, 16, 2 * toks), jnp.float32),
            pltpu.VMEM((steps, 2 * toks, rows_n), bf),
            pltpu.VMEM(group, bf),
            pltpu.VMEM(group, bf),
            pltpu.VMEM(group, bf),
            pltpu.VMEM((steps, rows_n, hidden), bf),
            pltpu.VMEM((steps, rows_n, hidden), bf),
            pltpu.VMEM((hidden, half), bf),
            pltpu.VMEM(group, bf),
            pltpu.VMEM(group, bf),
            pltpu.VMEM((steps, 2, toks, half), bf),
            pltpu.VMEM((steps, toks, half), bf),
            pltpu.VMEM((steps, toks, half), bf),
            dma((steps, 2)), dma((steps, 2)), dma((steps, 2)), dma((steps, 2)),
            dma((steps,)), dma((steps,)), dma((steps,)), dma((steps,)),
            dma((steps,)), dma((steps,)), dma, dma,
            dma((steps,)), dma((steps,)), dma((steps, 2)), dma((steps, 2)),
        ],
        compiler_params=pltpu.CompilerParams(
            collective_id=1, has_side_effects=True, vmem_limit_bytes=60 * 2**20
        ),
        name="routed_experts",
    )(meta, tokens, gate_weight, up_weight, down_weight)


def front_kernel(
    q_ref, cache_ref, bound_ref, pack_ref, res_ref, gain_ref, router_ref, ids_ref,
    hidden_ref, normed_ref, meta_ref,
    buf, cachex, bias, spread, wide, att, attx, full,
    r_sem, s_sem, c_s, c_r, o_s, o_r,
):
    x, x_up, x_down, nx = ring_ids("ep_0")
    z, z_up, z_down, nz = ring_ids("ep_1")
    core = lax.axis_index("tp")
    other = 1 - core
    toks = res_ref.shape[0]
    per_half = cache_ref.shape[1]
    latent = spread.shape[1]

    barrier = pltpu.get_barrier_semaphore()
    for name, peer in (
        ("ep_0", x_up), ("ep_0", x_down), ("ep_1", z_up), ("ep_1", z_down), ("tp", other)
    ):
        pl.semaphore_signal(barrier, inc=1, device_id={name: peer}, device_id_type=MESH)
    pl.semaphore_wait(barrier, 5)

    def send(a, xs, zs, axis, up, src=None):
        if axis == 0:
            name, peer = "ep_0", (x_up if up else x_down)
        else:
            name, peer = "ep_1", (z_up if up else z_down)
        here = buf.at[a, xs, zs]
        return pltpu.make_async_remote_copy(
            src_ref=here if src is None else src,
            dst_ref=here,
            send_sem=s_sem.at[a, axis, 0 if up else 1],
            recv_sem=r_sem.at[a, xs, zs],
            device_id={name: peer},
            device_id_type=MESH,
        )

    def arrived(a, xs, zs):
        wait_bytes(buf.at[a, xs, zs], r_sem.at[a, xs, zs])

    def at(a, first, second):
        xs, zs = (first, second) if a == 0 else (second, first)
        return lax.rem(xs + nx, nx), lax.rem(zs + nz, nz)

    spans = ((nx, nz), (nz, nx))
    places = ((x, z), (z, x))

    def start_own(a):
        src = pack_ref.at[a]
        for axis in (a, 1 - a):
            for up in (True, False):
                send(a, x, z, axis, up, src).start()

    def first_ring(a, t):
        (nf, _), (f, s) = spans[a], places[a]
        for up in (True, False):
            last = nf // 2 if up else nf // 2 - 1

            @pl.when((t >= 1) & (t <= last))
            def _(up=up, last=last):
                xs, zs = at(a, f - t if up else f + t, s)
                arrived(a, xs, zs)

                @pl.when(t < last)
                def _():
                    send(a, xs, zs, a, up).start()

                send(a, xs, zs, 1 - a, True).start()
                send(a, xs, zs, 1 - a, False).start()

    def second_ring(a, d, h):
        (nf, ns), (f, s) = spans[a], places[a]
        for below in (True, False):
            if below:
                held = (d >= 0) & (d <= nf // 2)
            else:
                held = (d >= 1) & (d <= nf // 2 - 1)
            for up in (True, False):
                last = ns // 2 if up else ns // 2 - 1

                @pl.when(held & (h >= 1) & (h <= last))
                def _(below=below, up=up, last=last):
                    xs, zs = at(a, f - d if below else f + d, s - h if up else s + h)
                    arrived(a, xs, zs)

                    @pl.when(h < last)
                    def _():
                        send(a, xs, zs, 1 - a, up).start()

    start_own(0)
    start_own(1)
    swap = pltpu.make_async_remote_copy(
        src_ref=cache_ref, dst_ref=cachex, send_sem=c_s, recv_sem=c_r,
        device_id={"tp": other}, device_id_type=MESH,
    )
    swap.start()
    for a in range(2):
        buf[a, x, z] = pack_ref[a]

    keys_n = bias.shape[2]
    column = lax.broadcasted_iota(jnp.int32, (toks, keys_n), 1)
    owner = column // per_half
    place = column % per_half
    limit = jnp.zeros((toks, keys_n), jnp.int32)
    for r in range(cache_ref.shape[0]):
        limit = jnp.where(owner == r, bound_ref[:, r : r + 1], limit)
    for half, index in ((0, core), (1, other)):
        bias[half] = jnp.where(place + index * per_half < limit, 0.0, -jnp.inf)
    source = lax.broadcasted_iota(jnp.int32, (latent, 2 * latent), 0)
    target = lax.broadcasted_iota(jnp.int32, (latent, 2 * latent), 1)
    for group in range(2):
        goal = (source // 4) * 8 + group * 4 + source % 4
        spread[group] = jnp.where(goal == target, 1.0, 0.0).astype(jnp.bfloat16)

    expert_n = router_ref.shape[1]
    experts = lax.broadcasted_iota(jnp.int32, (toks, expert_n), 1)
    named = [experts == ids_ref[:, k : k + 1] for k in range(TOPK)]

    def attend(p):
        queries = q_ref[pl.ds(2 * p, 2)].reshape(2 * toks, q_ref.shape[2])

        def scored(ref, half):
            keys = ref[...].reshape(keys_n, ref.shape[2])
            scores = lax.dot_general(
                queries, keys, (((1,), (1,)), ((), ())), preferred_element_type=jnp.float32
            )
            both = scores.reshape(2, toks, keys_n) * score_scale + bias[half][None]
            return both.reshape(2 * toks, keys_n)

        near = scored(cache_ref, 0)
        far = scored(cachex, 1)
        peak = jnp.maximum(
            jnp.max(near, axis=1, keepdims=True), jnp.max(far, axis=1, keepdims=True)
        )
        near = jnp.exp(near - peak).astype(jnp.bfloat16)
        far = jnp.exp(far - peak).astype(jnp.bfloat16)
        totals = jnp.sum(near.astype(jnp.float32), axis=1, keepdims=True) + jnp.sum(
            far.astype(jnp.float32), axis=1, keepdims=True
        )

        def summed(weights, ref):
            rows = ref[:, :, :latent].reshape(keys_n, latent)
            return jnp.dot(weights, rows, preferred_element_type=jnp.float32)

        context = ((summed(near, cache_ref) + summed(far, cachex)) / totals).astype(jnp.bfloat16)
        wide[p] = jnp.dot(
            context, spread[p % 2], preferred_element_type=jnp.float32
        ).astype(jnp.bfloat16)

    pieces = q_ref.shape[0] // 2
    ticks = nx // 2 + nz // 2 + 1

    def tick(t, carry):
        for a in range(2):
            first_ring(a, t)
        for d in range(nx // 2 + 1):
            second_ring(0, d, t - d)
        for h in range(1, nx // 2 + 1):
            second_ring(1, t - h, h)

        @pl.when((t >= 1) & (t <= pieces))
        def _():
            attend(t - 1)

        return carry

    swap.wait_recv()
    lax.fori_loop(0, ticks, tick, 0)
    for p in range(max(ticks - 1, 0), pieces):
        attend(p)

    columns = nx * nz * 16
    part = jnp.zeros((toks, columns), jnp.float32)
    for a in range(2):
        values = buf[a, :, :, 32:40, :].reshape(2 * latent, buf.shape[4])
        by_side = []
        for b in range(2):
            stacked = jnp.concatenate(
                [wide[2 * a + g, b * toks : (b + 1) * toks, :] for g in range(2)], axis=0
            )
            by_side.append(
                jnp.dot(
                    stacked, values[:, b * VDIM : (b + 1) * VDIM],
                    preferred_element_type=jnp.float32,
                ).astype(jnp.bfloat16)
            )
        for g in range(2):
            heads = jnp.concatenate(
                [side[g * toks : (g + 1) * toks] for side in by_side], axis=1
            )
            weights = buf[a, :, :, g * 16 : (g + 1) * 16, :].reshape(columns, buf.shape[4])
            part = part + lax.dot_general(
                heads, weights, (((1,), (1,)), ((), ())), preferred_element_type=jnp.float32
            )
    att[...] = part
    merge = pltpu.make_async_remote_copy(
        src_ref=att, dst_ref=attx, send_sem=o_s, recv_sem=o_r,
        device_id={"tp": other}, device_id_type=MESH,
    )
    merge.start()

    counts = jnp.zeros((toks, expert_n), jnp.float32)
    for hit in named:
        counts = counts + jnp.where(hit, 1.0, 0.0)
    token_a = lax.broadcasted_iota(jnp.int32, (toks, toks), 0)
    token_b = lax.broadcasted_iota(jnp.int32, (toks, toks), 1)
    before = jnp.where(token_b < token_a, 1.0, 0.0).astype(jnp.bfloat16)
    earlier = jnp.dot(before, counts.astype(jnp.bfloat16), preferred_element_type=jnp.float32)
    lane = lax.broadcasted_iota(jnp.int32, (toks, 128), 1)
    table = jnp.zeros((toks, 128), jnp.float32)
    for k, hit in enumerate(named):
        spot = jnp.sum(jnp.where(hit, earlier, 0.0), axis=1, keepdims=True)
        slot = ids_ref[:, k : k + 1].astype(jnp.float32) * CAP + spot
        table = jnp.where(lane == k, slot, table)

    merge.wait_recv()
    hidden = (res_ref[...].astype(jnp.float32) + (att[...] + attx[...])).astype(jnp.bfloat16)
    hidden_wide = hidden.astype(jnp.float32)
    square = jnp.mean(hidden_wide * hidden_wide, axis=1, keepdims=True)
    normed = (hidden_wide * lax.rsqrt(square + epsilon) * gain_ref[...]).astype(jnp.bfloat16)
    logits = jnp.dot(normed, router_ref[...], preferred_element_type=jnp.float32)
    chosen = [
        jnp.sum(jnp.where(hit, logits, 0.0), axis=1, keepdims=True) for hit in named
    ]
    top = functools.reduce(jnp.maximum, chosen)
    raised = [jnp.exp(value - top) for value in chosen]
    total = functools.reduce(jnp.add, raised)
    for k, value in enumerate(raised):
        share = (value / total).astype(jnp.bfloat16).astype(jnp.float32)
        table = jnp.where(lane == 8 + k, share, table)
    meta_ref[...] = jnp.concatenate([table, table], axis=0).T[:16]
    half_width = normed_ref.shape[1]
    mine = pl.ds(pl.multiple_of(core * half_width, half_width), half_width)
    full[0] = hidden
    full[1] = normed
    hidden_ref[...] = full[0, :, mine]
    normed_ref[...] = full[1, :, mine]

    swap.wait_send()
    merge.wait_send()
    for a in range(2):
        nf, ns = spans[a]
        for up in (0, 1):
            if a == 0:
                wait_bytes(buf.at[0, pl.ds(0, nf // 2 - up), 0], s_sem.at[0, 0, up])
                wait_bytes(buf.at[0, :, pl.ds(0, ns // 2 - up)], s_sem.at[0, 1, up])
            else:
                wait_bytes(buf.at[1, 0, pl.ds(0, nf // 2 - up)], s_sem.at[1, 1, up])
                wait_bytes(buf.at[1, pl.ds(0, ns // 2 - up)], s_sem.at[1, 0, up])


def attention_front(
    queries, latent_cache, residual, token_request, token_visible,
    value_proj, out_proj, norm_gain, router, expert_ids,
):
    nx, nz = lax.axis_size("ep_0"), lax.axis_size("ep_1")
    toks, heads, width = queries.shape
    requests, per_half, _ = latent_cache.shape
    model = residual.shape[1]
    latent = value_proj.shape[1] * nx * nz
    bf, f32 = jnp.bfloat16, jnp.float32
    quarter = heads // 4 * VDIM
    out_rows = out_proj.reshape(4, quarter, -1).transpose(0, 2, 1).reshape(2, 32, quarter)
    value_rows = value_proj.reshape(2, 2, 2, 4, VDIM).transpose(0, 1, 3, 2, 4)
    pack = jnp.concatenate([out_rows, value_rows.reshape(2, 8, quarter)], axis=1)
    request = jnp.arange(requests, dtype=jnp.int32)
    bound = jnp.where(token_request[:, None] == request, token_visible[:, None], 0)
    dma = pltpu.SemaphoreType.DMA
    half = model // lax.axis_size("tp")
    return pl.pallas_call(
        front_kernel,
        out_shape=(
            jax.ShapeDtypeStruct((toks, half), bf),
            jax.ShapeDtypeStruct((toks, half), bf),
            jax.ShapeDtypeStruct((16, 2 * toks), f32),
        ),
        in_specs=[pl.BlockSpec(memory_space=pltpu.VMEM)] * 8,
        out_specs=(pl.BlockSpec(memory_space=pltpu.VMEM),) * 3,
        scratch_shapes=[
            pltpu.VMEM((2, nx, nz, 40, quarter), bf),
            pltpu.VMEM(latent_cache.shape, bf),
            pltpu.VMEM((2, toks, requests * per_half), f32),
            pltpu.VMEM((2, latent, 2 * latent), bf),
            pltpu.VMEM((heads // 2, 2 * toks, 2 * latent), bf),
            pltpu.VMEM((toks, model), f32),
            pltpu.VMEM((toks, model), f32),
            pltpu.VMEM((2, toks, model), bf),
            dma((2, nx, nz)), dma((2, 2, 2)), dma, dma, dma, dma,
        ],
        compiler_params=pltpu.CompilerParams(
            collective_id=2, has_side_effects=True, vmem_limit_bytes=60 * 2**20
        ),
        name="attention_front",
    )(
        queries.transpose(1, 0, 2), latent_cache, bound, pack, residual,
        norm_gain.reshape(1, model), router, expert_ids,
    )


def body(
    queries,
    latent_cache,
    residual,
    token_request,
    token_visible,
    value_proj,
    out_proj,
    norm_gain,
    router,
    expert_ids,
    gate_weight,
    up_weight,
    down_weight,
):
    hidden_part, normed_part, meta = attention_front(
        queries, latent_cache, residual, token_request, token_visible,
        value_proj, out_proj, norm_gain, router, expert_ids,
    )
    expert_out = routed_experts(
        meta, normed_part, gate_weight[0], up_weight[0], down_weight[0]
    )
    return (hidden_part, expert_out)


def solution(mesh):
    finer = Mesh(
        mesh.devices.reshape(mesh.shape["grp"], 8, 16, mesh.shape["tp"]),
        ("grp", "ep_0", "ep_1", "tp"),
    )
    in_specs = (
        P(GRP_EP, "tp", None),
        P(GRP_EP, "tp", None),
        P(GRP_EP, None),
        P(GRP_EP),
        P(GRP_EP),
        P("tp", EP, None),
        P("tp", EP),
        P(),
        P(),
        P(GRP_EP, None),
        P(EP, None, "tp"),
        P(EP, None, "tp"),
        P(EP, "tp", None),
    )
    out_specs = (P(GRP_EP, "tp"), P(GRP_EP, "tp"))
    return jax.shard_map(body, mesh=finer, in_specs=in_specs, out_specs=out_specs, check_vma=False)
```
